32 devices in a mesh: blk: 32 (over z, y, x, core).
Axes of the slice: x: 2, y: 2, z: 4, core: 2. Of those that a mesh axis runs over, the one named last changes fastest.
Arguments:
- wannier: bfloat16 [64, 110592], P('blk'), may hold values from -6 to 6
- pairs: int32 [32, 2, 1, 6], P('blk'), may hold values from 0 to 24, as said below
Outputs:
- exchange_image: bfloat16 [64, 110592], P('blk')
The draws below stay inside these ranges and needn't reach their ends.
Inputs may be any that keep to these rules, and one draw needn't show every extreme that they name: `pairs`: columns 0 and 1 lie in 0..1, columns 2 to 4 in 0..24, column 5 is 0 or 1; some device has all 1 slots live in every step.
All inputs are finite; a program needn't handle non-finite values.
Results may differ from the reference program's by a relative error of at most 0.00125.
Values may be sent and summed in bfloat16 or wider, within the bound.
No kernel may reach another device: no remote copies, remote signals or barrier semaphores. Data moves between devices by JAX's collectives and lax.ppermute only.
A program may use at most 64 MiB of HBM per device.

```python
import jax
import jax.numpy as jnp
from jax import lax

G = 48
NW_DEV = 2
STEPS = 2
SLOTS = 1
P_SIZE = 96
E = 72
NWALL = 64
N_BLK = 32


def draw_pairs(key, part):
    keys = jax.random.split(jax.random.fold_in(key, 17), 4)
    shape = (N_BLK, STEPS, SLOTS)
    resident = jax.random.randint(keys[0], shape, 0, NW_DEV)
    visiting = jax.random.randint(keys[1], shape, 0, NW_DEV)
    offsets = jax.random.randint(keys[2], shape + (3,), 0, G // 2 + 1)
    coin = jax.random.randint(keys[3], shape, 0, 5)
    live = jnp.where(coin < 4, 1, 0)
    first = jnp.arange(N_BLK)[:, None, None] == 0
    live = jnp.where(first, 1, live)
    stacked = jnp.concatenate([resident[..., None], visiting[..., None], offsets, live[..., None]], axis=-1)
    return stacked.astype(jnp.int32)


def shard_levels(key, extent, pieces, least, top_value):
    def one(axis_at, blocks):
        draws = jax.random.uniform(jax.random.fold_in(jax.random.fold_in(key, 6), axis_at), (blocks,), jnp.float32, least / len(pieces), top_value / len(pieces))
        return jnp.repeat(jnp.exp(draws), extent[axis_at] // blocks).reshape((-1,) + (1,) * (len(extent) - axis_at - 1))

    factor_of = one(*pieces[0])
    for cut in pieces[1:]:
        factor_of = factor_of * one(*cut)
    return factor_of


def gaussian(own_key, dims, spread, limit, pieces=(), held_as=jnp.bfloat16):
    result = jax.random.normal(own_key, dims, jnp.float32) * spread
    if len(pieces) > 0:
        result = shard_levels(own_key, dims, pieces, -0.22, 0.18) * result
    return jnp.clip(result, min=-limit, max=limit).astype(held_as)


def setup_inputs(seed: int = 0) -> dict:
    streams_of = jax.random.split(jax.random.key(seed), 3)
    return {
        "wannier": gaussian(streams_of[0], (NWALL, G * G * G), 1.0, 6.0, ((0, 32),)),
        "pairs": draw_pairs(jax.random.fold_in(streams_of[2], 71), 0),
    }


def sine_tables():
    index = jnp.arange(P_SIZE, dtype=jnp.float32) + 1.0
    sine = jnp.sqrt(2.0 / (P_SIZE + 1.0)) * jnp.sin(jnp.pi * index[:, None] * index[None, :] / (P_SIZE + 1.0))
    single = 2.0 - 2.0 * jnp.cos(jnp.pi * index / (P_SIZE + 1.0))
    lam = single[:, None, None] + single[None, :, None] + single[None, None, :]
    return (sine, 1.0 / lam)

def pair_terms(resident, visiting, entry, sine, inv_lam):
    high = lax.Precision.HIGHEST
    res = resident.astype(jnp.float32).reshape(G, G, G)
    vis = visiting.astype(jnp.float32).reshape(G, G, G)
    res_e = jnp.pad(res, ((0, E - G), (0, E - G), (0, E - G)))
    vis_e = lax.dynamic_update_slice(jnp.zeros((E, E, E), jnp.float32), vis, (entry[2].astype(jnp.int32), entry[3].astype(jnp.int32), entry[4].astype(jnp.int32)))
    rho = (res_e * vis_e)[:G, :G, :G]
    part_sine = sine[:, :G]
    hat = jnp.einsum('ai,ijk->ajk', part_sine, rho, precision=high)
    hat = jnp.einsum('bj,ajk->abk', part_sine, hat, precision=high)
    hat = jnp.einsum('ck,abk->abc', part_sine, hat, precision=high)
    hat = hat * inv_lam
    back_sine = sine[:E, :]
    phi = jnp.einsum('ia,abc->ibc', back_sine, hat, precision=high)
    phi = jnp.einsum('jb,ibc->ijc', back_sine, phi, precision=high)
    phi = jnp.einsum('kc,ijc->ijk', back_sine, phi, precision=high)
    live = entry[5].astype(jnp.float32)
    to_resident = (phi * vis_e)[:G, :G, :G] * live
    to_visiting = lax.dynamic_slice(phi * res_e, (entry[2].astype(jnp.int32), entry[3].astype(jnp.int32), entry[4].astype(jnp.int32)), (G, G, G)) * live
    return (to_resident.reshape(G * G * G), to_visiting.reshape(G * G * G))

def reference(wannier, pairs):
    sine, inv_lam = sine_tables()
    device = jnp.arange(N_BLK, dtype=jnp.int32)[:, None, None]
    step = jnp.arange(1, STEPS + 1, dtype=jnp.int32)[None, :, None]
    owner_res = device * NW_DEV + pairs[..., 0].astype(jnp.int32)
    owner_vis = (device - step) % N_BLK * NW_DEV + pairs[..., 1].astype(jnp.int32)
    flat_res = owner_res.reshape(-1)
    flat_vis = owner_vis.reshape(-1)
    flat_entry = pairs.reshape(-1, 6).astype(jnp.int32)

    def visit(total, item):
        index_res, index_vis, entry = item
        to_resident, to_visiting = pair_terms(wannier[index_res], wannier[index_vis], entry, sine, inv_lam)
        total = total.at[index_res].add(to_resident)
        total = total.at[index_vis].add(to_visiting)
        return (total, None)
    start = jnp.zeros((NWALL, G * G * G), jnp.float32)
    total, unused = lax.scan(visit, start, (flat_res, flat_vis, flat_entry))
    return total.astype(jnp.bfloat16)
```

```python
import functools

import jax
import jax.numpy as jnp
import numpy as np
from jax import lax
from jax.experimental import pallas as pl
from jax.experimental.pallas import tpu as pltpu
from jax.sharding import PartitionSpec as P

LANES = 128
VMEM_BYTES = 20 * 1024 * 1024


class Plan:
    def __init__(self, points):
        self.g = g = round(points ** (1.0 / 3.0))
        assert g**3 == points and (g * g) % (2 * LANES) == 0 and g % 16 == 0
        self.modes = 2 * g
        assert self.modes <= LANES
        self.tiles = g * g // LANES
        self.rows = points // LANES
        span = int(np.lcm(g, LANES))
        self.js = span // g
        self.us = span // LANES
        self.groups = self.tiles // self.us
        half = g // 2
        self.pad = -(-(half * (g * g + g + 1) // LANES + 1) // 8) * 8
        self.blocks = [
            (j, u)
            for j in range(self.js)
            for u in range(self.us)
            if j * g < (u + 1) * LANES and (j + 1) * g > u * LANES
        ]
        self.block_of = {pair: at for at, pair in enumerate(self.blocks)}


def split_np(x):
    hi_np = np.asarray(x, np.float32).astype(jnp.bfloat16)
    lo_np = (np.asarray(x, np.float64) - hi_np.astype(np.float64)).astype(jnp.bfloat16)
    return hi_np, lo_np


def constants(plan):
    g, m = plan.g, plan.modes
    index = np.arange(m, dtype=np.float64) + 1.0
    sine = np.sqrt(2.0 / (m + 1.0)) * np.sin(np.pi * index[:, None] * index[None, :] / (m + 1.0))
    single = 2.0 - 2.0 * np.cos(np.pi * index / (m + 1.0))
    hi, lo = split_np(sine[:, :g])
    first = np.concatenate([hi, hi, lo], axis=1)
    last = np.concatenate(
        [np.concatenate([hi.T, hi.T], axis=1), np.concatenate([lo.T, lo.T], axis=1)], axis=0
    )
    forward, backward = [], []
    for j, u in plan.blocks:
        placed = np.zeros((LANES, LANES), np.float64)
        for lane in range(LANES):
            k = u * LANES + lane - j * g
            if 0 <= k < g:
                placed[lane, :m] = sine[:, k]
        forward.append(np.stack(split_np(placed)))
        backward.append(np.stack(split_np(placed.T)))
    mu = np.ones((m, LANES), np.float64)
    mu[:, :m] = single[:, None] + single[None, :]
    return (
        first,
        last,
        np.stack(forward),
        np.stack(backward),
        mu.astype(np.float32),
    )


def split(x):
    hi = x.astype(jnp.bfloat16)
    lo = (x - hi.astype(jnp.float32)).astype(jnp.bfloat16)
    return hi, lo


def dot(a, b):
    return jnp.dot(a, b, preferred_element_type=jnp.float32)


def ratio_kernel(plan, mu_ref, out_ref):
    mu = mu_ref[...]
    small = jnp.ones_like(mu)
    for j in range(plan.g):
        before = small
        total = mu + small
        ratio = 1.0 / (1.0 + total)
        small = total * ratio
        if j == plan.g - 1:
            ratio = 1.0 / (mu + before + small)
        out_ref[j] = ratio


def pick_kernel(column, e1_ref, e2_ref, w_ref, o1_ref, o2_ref):
    o1_ref[...] = w_ref[e1_ref[0, 0, 0, column]]
    o2_ref[...] = w_ref[e2_ref[0, 1, 0, column]]


def solve_kernel(
    plan, owner, step, final, *refs
):
    (e_ref, w_ref, x_ref, first_ref, last_ref, fwd_ref, bwd_ref, ratio_ref) = refs[:8]
    refs = refs[8:]
    if final:
        others, refs = refs[:5], refs[5:]
    out_ref, a_pad, b_pad, b_sh, xs, z, ys, v = refs[:8]
    g, m = plan.g, plan.modes
    r_at = e_ref[0, step, 0, 0]
    v_at = e_ref[0, step, 0, 1]
    ox = e_ref[0, step, 0, 2]
    oy = e_ref[0, step, 0, 3]
    oz = e_ref[0, step, 0, 4]
    live = e_ref[0, step, 0, 5].astype(jnp.float32)
    shift = ox * (g * g) + oy * g + oz
    down = lax.shift_right_logical(shift, 7)
    roll = shift & (LANES - 1)

    if owner:
        a_pad[: plan.rows, :] = x_ref[...].astype(jnp.float32)
        b_pad[plan.pad :, :] = w_ref[v_at].astype(jnp.float32)
    else:
        a_pad[: plan.rows, :] = w_ref[r_at].astype(jnp.float32)
        b_pad[plan.pad :, :] = x_ref[...].astype(jnp.float32)
    b_pad[: plan.pad, :] = jnp.zeros((plan.pad, LANES), jnp.float32)

    lane = lax.broadcasted_iota(jnp.int32, (8, LANES), 1)

    def j_and_k(t):
        flat = (lane + t * LANES).astype(jnp.float32)
        j = jnp.floor((flat + 0.5) * (1.0 / g))
        return j.astype(jnp.int32), (flat - j * g).astype(jnp.int32)

    def tall(x):
        return jnp.concatenate([x] * (g // 8), axis=0)

    def moved(ref, start, amount):
        return pltpu.roll(ref[pl.ds(start, g, stride=plan.tiles), :], amount, 1)

    from_before = tall(lane < roll)
    before = moved(b_pad, plan.pad - 1 - down, roll)
    for pair in range(plan.tiles // 2):
        rhs = []
        for t in (2 * pair, 2 * pair + 1):
            here = moved(b_pad, plan.pad + t - down, roll)
            j, k = j_and_k(t)
            valid = tall((j >= oy) & (k >= oz))
            b = jnp.where(valid, jnp.where(from_before, before, here), 0.0)
            before = here
            if not owner:
                b_sh[t] = b
            rho = a_pad[pl.ds(t, g, stride=plan.tiles), :] * b
            hi, lo = split(rho)
            rhs.append(jnp.concatenate([hi, lo, hi], axis=0))
        x = dot(first_ref[...], jnp.concatenate(rhs, axis=1))
        for side in range(2):
            t = 2 * pair + side
            at, u = divmod(t, plan.us)
            hi, lo = split(x[:, side * LANES : (side + 1) * LANES])
            rows = pl.ds(at * m, m)
            xs[rows, pl.ds(2 * u * LANES, LANES)] = hi
            xs[rows, pl.ds((2 * u + 1) * LANES, LANES)] = lo

    zero = jnp.zeros((LANES, LANES), jnp.bfloat16)

    def placed(j, u, part):
        at = plan.block_of.get((j, u))
        return zero if at is None else fwd_ref[at, part]

    for p in range(plan.js // 2):
        us = [u for u in range(plan.us) if (2 * p, u) in plan.block_of or (2 * p + 1, u) in plan.block_of]
        lows_l, lows_r, total = [], [], None
        for u in us:
            high = jnp.concatenate([placed(2 * p, u, 0), placed(2 * p + 1, u, 0)], axis=1)
            lows_r.append(jnp.concatenate([placed(2 * p, u, 1), placed(2 * p + 1, u, 1)], axis=1))
            lows_l.append(xs[:, pl.ds(2 * u * LANES, LANES)])
            term = dot(xs[:, pl.ds(2 * u * LANES, 2 * LANES)], jnp.concatenate([high, high], axis=0))
            total = term if total is None else total + term
        total = total + dot(jnp.concatenate(lows_l, axis=1), jnp.concatenate(lows_r, axis=0))
        for at in range(plan.groups):
            for h in range(2):
                z[plan.js * at + 2 * p + h] = total[at * m : (at + 1) * m, h * LANES : (h + 1) * LANES]

    w = z[0]
    for j in range(1, g):
        w = z[j] + ratio_ref[j - 1] * w
        z[j] = w
    y = jnp.zeros((m, LANES), jnp.float32)
    for j in reversed(range(g)):
        y = ratio_ref[j] * (z[j] + y)
        at, jl = divmod(j, plan.js)
        hi, lo = split(y)
        ys[jl, pl.ds(at * m, m), pl.ds(0, LANES)] = hi
        ys[jl, pl.ds(at * m, m), pl.ds(LANES, LANES)] = lo

    for u in range(plan.us):
        total = None
        for j in range(plan.js):
            if (j, u) not in plan.block_of:
                continue
            at = plan.block_of[(j, u)]
            wide = jnp.concatenate([bwd_ref[at, 0], bwd_ref[at, 1]], axis=1)
            term = dot(ys[j], jnp.concatenate([wide, wide], axis=0))
            total = term if total is None else total + term
        total = total[:, :LANES] + total[:, LANES:]
        hi, lo = split(total)
        for at in range(plan.groups):
            t = plan.us * at + u
            rows = slice(at * m, (at + 1) * m)
            v[t // 2, pl.ds(0, m), pl.ds((t % 2) * LANES, LANES)] = hi[rows]
            v[t // 2, pl.ds(m, m), pl.ds((t % 2) * LANES, LANES)] = lo[rows]

    if owner:
        a_pad2 = b_pad
        a_pad2[plan.rows :, :] = jnp.zeros((plan.pad, LANES), jnp.float32)
    for pair in range(plan.tiles // 2):
        both = dot(last_ref[...], v[pair])
        phi2 = (both[:g] + both[g:]) * live
        for side in range(2):
            t = 2 * pair + side
            phi = phi2[:, side * LANES : (side + 1) * LANES]
            if owner:
                a_pad2[pl.ds(t, g, stride=plan.tiles), :] = phi * a_pad[pl.ds(t, g, stride=plan.tiles), :]
            elif not final:
                out_ref[t] = phi * b_sh[t]
            else:
                b_sh[t] = phi * b_sh[t]

    if owner:
        back = (LANES - roll) & (LANES - 1)
        from_here = tall(lane < LANES - roll)
        here = moved(a_pad2, down, back)
        for t in range(plan.tiles):
            after = moved(a_pad2, t + 1 + down, back)
            j, k = j_and_k(t)
            valid = tall((j < g - oy) & (k < g - oz))
            out_ref[t] = jnp.where(valid, jnp.where(from_here, here, after), 0.0)
            here = after
    if final:
        e1_ref, e2_ref, t1_ref, t2_ref, t3_ref = others
        places = [e1_ref[0, 0, 0, 1], e2_ref[0, 1, 0, 1], e_ref[0, 0, 0, 0], r_at]
        for f in range(2):
            for t in range(plan.tiles):
                total = jnp.zeros((g, LANES), jnp.float32)
                for place, term in zip(places, (t1_ref, t2_ref, t3_ref, b_sh)):
                    total = total + jnp.where(place == f, term[t], 0.0)
                a_pad[pl.ds(t, g, stride=plan.tiles), :] = total
            out_ref[f] = a_pad[...].astype(jnp.bfloat16)


def smem():
    return pl.BlockSpec(memory_space=pltpu.SMEM)


def vmem():
    return pl.BlockSpec(memory_space=pltpu.VMEM)


def params():
    return pltpu.CompilerParams(vmem_limit_bytes=VMEM_BYTES)


def cost(flops, size):
    return pl.CostEstimate(flops=flops, bytes_accessed=size, transcendentals=0)


def pick(plan, column, e1, e2, w):
    shape = jax.ShapeDtypeStruct(w.shape[1:], w.dtype)
    return pl.pallas_call(
        functools.partial(pick_kernel, column),
        out_shape=(shape, shape),
        in_specs=[smem(), smem(), vmem()],
        out_specs=(vmem(), vmem()),
        compiler_params=params(),
        cost_estimate=cost(10**6, 10**6),
        name="pick",
    )(e1, e2, w)


def solve(plan, owner, step, e, w, x, tables, others=None):
    g, m = plan.g, plan.modes
    final = others is not None
    if final:
        out = jax.ShapeDtypeStruct(w.shape, w.dtype)
    else:
        out = jax.ShapeDtypeStruct((plan.tiles, g, LANES), jnp.float32)
    extra = list(others) if final else []
    return pl.pallas_call(
        functools.partial(solve_kernel, plan, owner, step, final),
        out_shape=out,
        in_specs=[smem()] + [vmem()] * 7 + ([smem()] * 2 + [vmem()] * 3 if final else []),
        out_specs=vmem(),
        scratch_shapes=[
            pltpu.VMEM((plan.rows, LANES), jnp.float32),
            pltpu.VMEM((plan.rows + plan.pad, LANES), jnp.float32),
            pltpu.VMEM((plan.tiles, g, LANES), jnp.float32),
            pltpu.VMEM((plan.groups * m, 2 * plan.us * LANES), jnp.bfloat16),
            pltpu.VMEM((g, m, LANES), jnp.float32),
            pltpu.VMEM((plan.js, plan.groups * m, 2 * LANES), jnp.bfloat16),
            pltpu.VMEM((plan.tiles // 2, 2 * m, 2 * LANES), jnp.bfloat16),
        ],
        compiler_params=params(),
        cost_estimate=cost(2 * 10**8, 4 * 10**6),
        name="solve_owner" if owner else "solve_resident",
    )(e, w, x, *tables, *extra)


def per_device(wannier, pairs):
    plan = Plan(wannier.shape[1])
    count = lax.axis_size("blk")

    def shifted(array, by):
        return lax.ppermute(array, "blk", [(i, (i + by) % count) for i in range(count)])

    e1 = shifted(pairs, -1)
    e2 = shifted(pairs, -2)
    w = wannier.reshape(wannier.shape[0], plan.rows, LANES)
    a1, a2 = pick(plan, 0, pairs, pairs, w)
    a1 = shifted(a1, -1)
    a2 = shifted(a2, -2)
    b1, b2 = pick(plan, 1, e1, e2, w)
    b1 = shifted(b1, 1)
    b2 = shifted(b2, 2)
    first, last, fwd, bwd, mu = constants(plan)
    ratio = pl.pallas_call(
        functools.partial(ratio_kernel, plan),
        out_shape=jax.ShapeDtypeStruct((plan.g, plan.modes, LANES), jnp.float32),
        in_specs=[vmem()],
        out_specs=vmem(),
        compiler_params=params(),
        cost_estimate=cost(10**7, 10**6),
        name="ratios",
    )(mu)
    tables = (first, last, fwd, bwd, ratio)
    t1 = solve(plan, True, 0, e1, w, a1, tables)
    t2 = solve(plan, True, 1, e2, w, a2, tables)
    t3 = solve(plan, False, 0, pairs, w, b1, tables)
    out = solve(plan, False, 1, pairs, w, b2, tables, (e1, e2, t1, t2, t3))
    return out.reshape(wannier.shape)


def solution(mesh):
    return jax.shard_map(
        per_device,
        mesh=mesh,
        in_specs=(P("blk", None), P("blk", None, None, None)),
        out_specs=P("blk", None),
        check_vma=False,
    )
```

```python
import functools

import jax
import jax.numpy as jnp
import numpy as np
from jax import lax
from jax.experimental import pallas as pl
from jax.experimental.pallas import tpu as pltpu
from jax.sharding import PartitionSpec as P


LANES = 128
VMEM_BYTES = 20 * 1024 * 1024
PREP_BYTES = 64380928
PREP_CHUNKS = 4


class Plan:
    def __init__(self, points):
        self.g = g = round(points ** (1.0 / 3.0))
        assert g**3 == points and (g * g) % (2 * LANES) == 0 and g % 16 == 0
        self.modes = 2 * g
        assert self.modes <= LANES
        self.tiles = g * g // LANES
        self.rows = points // LANES
        half = g // 2
        self.pad = -(-(half * (g * g + g + 1) // LANES + 1) // 8) * 8


def split(x):
    hi = x.astype(jnp.bfloat16)
    lo = (x - hi.astype(jnp.float32)).astype(jnp.bfloat16)
    return hi, lo


def dot(a, b):
    return jnp.dot(a, b, preferred_element_type=jnp.float32)


def sine_table(shape, modes, row_end, lane_end):
    row = lax.broadcasted_iota(jnp.int32, shape, 0)
    lane = lax.broadcasted_iota(jnp.int32, shape, 1)
    period = 2 * (modes + 1)
    product = ((row + 1) * (lane + 1)).astype(jnp.float32)
    turns = jnp.floor((product + 0.5) * (1.0 / period))
    angle = (product - turns * period) * (np.pi / (modes + 1))
    sine = jnp.sin(angle) * np.sqrt(2.0 / (modes + 1.0))
    return jnp.where((row < row_end) & (lane < lane_end), sine, 0.0)


def tables_kernel(plan, start_ref, first_ref, last_ref, end_ref, ratio_ref):
    g, m = plan.g, plan.modes
    half = LANES // 2
    shape = (m, LANES)
    step = np.pi / (m + 1)
    row = lax.broadcasted_iota(jnp.int32, shape, 0).astype(jnp.float32)
    lane = lax.broadcasted_iota(jnp.int32, shape, 1).astype(jnp.float32)
    mu = 4.0 * (jnp.sin((row + 1.0) * (0.5 * step)) ** 2 + jnp.sin((lane + 1.0) * (0.5 * step)) ** 2)
    small = jnp.ones_like(mu)
    for j in range(g):
        before = small
        total = mu + small
        ratio = 1.0 / (1.0 + total)
        small = total * ratio
        if j == g - 1:
            ratio = 1.0 / (mu + before + small)
        ratio_ref[j] = ratio
    hi, lo = split(sine_table((m, LANES), m, m, g)[:, :g])
    first_ref[...] = jnp.concatenate([hi, hi, lo], axis=1)
    hi, lo = split(sine_table((g, LANES), m, g, m))
    gap = jnp.zeros((half - g, 2 * LANES), jnp.bfloat16)
    wide = jnp.concatenate([hi, lo], axis=1)
    start_ref[...] = jnp.concatenate([wide, gap, wide, gap], axis=0)
    end_ref[...] = jnp.concatenate(
        [jnp.concatenate([hi, hi], axis=1), jnp.concatenate([lo, lo], axis=1)], axis=0
    )
    hi, lo = hi[:, :m], lo[:, :m]
    last_ref[...] = jnp.concatenate(
        [jnp.concatenate([hi, hi], axis=1), jnp.concatenate([lo, lo], axis=1)], axis=0
    )


def prepare_kernel(plan, chunks, e_hbm, raw_hbm, w_ref, o1_ref, o2_ref, e_ref, raw_ref, both, sems):
    rows = plan.rows // chunks
    copies = [
        pltpu.make_async_copy(
            raw_hbm.at[pl.ds(2 * rows * at, 2 * rows)], raw_ref.at[pl.ds(2 * rows * at, 2 * rows)], sems.at[at]
        )
        for at in range(chunks)
    ]
    copies.append(pltpu.make_async_copy(e_hbm, e_ref, sems.at[chunks]))
    for copy in copies[-1:] + copies[:-1]:
        copy.start()
    copies[-1].wait()
    first = e_ref[0, 0, 0, 0] == 0
    second = e_ref[0, 1, 0, 0] == 0
    for at in range(chunks):
        copies[at].wait()
        here = pl.ds(rows * at, rows)
        both[pl.ds(2 * rows * at, 2 * rows), :] = raw_ref[pl.ds(2 * rows * at, 2 * rows), :].astype(jnp.float32)
        f0, f1 = [both[pl.ds(2 * rows * at + f, rows, stride=2), :] for f in range(2)]
        w_ref[0, here, :] = f0.astype(jnp.bfloat16)
        w_ref[1, here, :] = f1.astype(jnp.bfloat16)
        o1_ref[here, :] = jnp.where(first, f0, f1).astype(jnp.bfloat16)
        o2_ref[here, :] = jnp.where(second, f0, f1).astype(jnp.bfloat16)


def pick_kernel(step, e_ref, w_ref, out_ref):
    out_ref[...] = w_ref[e_ref[0, step, 0, 1]]


def solve_kernel(plan, role, step, *refs):
    owner = role.startswith("visiting")
    (e_ref, w_ref, x_ref, start_ref, first_ref, last_ref, end_ref, ratio_ref) = refs[:8]
    refs = refs[8:]
    if role == "visiting_sum":
        (other_e_ref, other_ref), refs = refs[:2], refs[2:]
    if role == "last":
        (partial_ref, other_ref), refs = refs[:2], refs[2:]
    out_ref, a_pad, b_pad, b_sh, rho_t, x_hi, x_lo, z, y_hi, y_lo, v = refs[:11]
    both = refs[11] if role == "last" else None
    g, m = plan.g, plan.modes
    r_at = e_ref[0, step, 0, 0]
    v_at = e_ref[0, step, 0, 1]
    ox = e_ref[0, step, 0, 2]
    oy = e_ref[0, step, 0, 3]
    oz = e_ref[0, step, 0, 4]
    live = e_ref[0, step, 0, 5].astype(jnp.float32)
    shift = ox * (g * g) + oy * g + oz
    down = lax.shift_right_logical(shift, 7)
    roll = shift & (LANES - 1)

    if owner:
        a_pad[: plan.rows, :] = x_ref[...].astype(jnp.float32)
        b_pad[plan.pad :, :] = w_ref[v_at].astype(jnp.float32)
    else:
        a_pad[: plan.rows, :] = w_ref[r_at].astype(jnp.float32)
        b_pad[plan.pad :, :] = x_ref[...].astype(jnp.float32)
    b_pad[: plan.pad, :] = jnp.zeros((plan.pad, LANES), jnp.float32)

    lane = lax.broadcasted_iota(jnp.int32, (8, LANES), 1)

    def j_and_k(t):
        flat = (lane + t * LANES).astype(jnp.float32)
        j = jnp.floor((flat + 0.5) * (1.0 / g))
        return j.astype(jnp.int32), (flat - j * g).astype(jnp.int32)

    def tall(x):
        return jnp.concatenate([x] * (g // 8), axis=0)

    def moved(ref, start, amount):
        return pltpu.roll(ref[pl.ds(start, g, stride=plan.tiles), :], amount, 1)

    from_before = tall(lane < roll)
    parts = 3
    js = g // parts
    tiles = plan.tiles // parts
    assert g % parts == 0 and js % 2 == 0 and plan.tiles % parts == 0 and tiles % 2 == 0
    last_rolled = [moved(b_pad, plan.pad - 1 - down, roll)]
    gap = jnp.zeros((LANES // 2 - g, LANES), jnp.bfloat16)

    def shift_and_start(part):
        for t in range(part * tiles, (part + 1) * tiles):
            before = last_rolled[0]
            here = moved(b_pad, plan.pad + t - down, roll)
            j, k = j_and_k(t)
            valid = tall((j >= oy) & (k >= oz))
            b = jnp.where(valid, jnp.where(from_before, before, here), 0.0)
            last_rolled[0] = here
            if not owner:
                b_sh[t] = b
            hi, lo = split(a_pad[pl.ds(t, g, stride=plan.tiles), :] * b)
            rho_t[pl.ds(t * LANES, LANES), :] = jnp.concatenate([hi, gap, lo, gap], axis=0).T
            if t % 2:
                rows = pl.ds((t - 1) * LANES, 2 * LANES)
                x = dot(rho_t[rows, :], start_ref[...])
                x_hi[rows, :], x_lo[rows, :] = split(x[:, :LANES] + x[:, LANES:])

    def beside(ref, j, rows):
        return jnp.concatenate([ref[pl.ds(j * rows, rows), :], ref[pl.ds((j + 1) * rows, rows), :]], axis=1)

    def first(part):
        for j in range(part * js, (part + 1) * js, 2):
            hi, lo = beside(x_hi, j, g), beside(x_lo, j, g)
            x = dot(first_ref[...], jnp.concatenate([hi, lo, hi], axis=0))
            z[j], z[j + 1] = x[:, :LANES], x[:, LANES:]

    swept = [None]

    def sweep_up(part):
        w = swept[0]
        for j in range(part * js, (part + 1) * js):
            w = z[j] if j == 0 else z[j] + ratio_ref[j - 1] * w
            z[j] = w
        swept[0] = w

    def sweep_down(part):
        y = swept[0]
        for j in reversed(range(part * js, (part + 1) * js)):
            y = ratio_ref[j] * (z[j] + y)
            y_hi[pl.ds(j * m, m), :], y_lo[pl.ds(j * m, m), :] = split(y)
        swept[0] = y

    def last(part):
        for j in reversed(range(part * js, (part + 1) * js, 2)):
            x = dot(last_ref[...], jnp.concatenate([beside(y_hi, j, m), beside(y_lo, j, m)], axis=0))
            hi, lo = split(x[:g] + x[g:])
            for side in range(2):
                rows = pl.ds((j + side) * g, g)
                lanes = slice(side * LANES, (side + 1) * LANES)
                v[rows, pl.ds(0, LANES)] = hi[:, lanes]
                v[rows, pl.ds(LANES, LANES)] = lo[:, lanes]

    def end(part):
        for pair in range(part * tiles // 2, (part + 1) * tiles // 2):
            pieces = lax.dot_general(
                end_ref[...],
                v[pl.ds(pair * 2 * LANES, 2 * LANES), :],
                (((1,), (1,)), ((), ())),
                preferred_element_type=jnp.float32,
            )
            phi2 = (pieces[:g] + pieces[g:]) * live
            for side in range(2):
                t = 2 * pair + side
                phi = phi2[:, side * LANES : (side + 1) * LANES]
                if owner:
                    b_pad[pl.ds(t, g, stride=plan.tiles), :] = phi * a_pad[pl.ds(t, g, stride=plan.tiles), :]
                elif role == "resident":
                    out_ref[t] = phi * b_sh[t]
                else:
                    own, other = phi * b_sh[t], other_ref[t]
                    other_at = e_ref[0, 0, 0, 0]
                    for f in range(2):
                        total = partial_ref[f, t]
                        total = total + jnp.where(other_at == f, other, 0.0) + jnp.where(r_at == f, own, 0.0)
                        both[pl.ds(2 * t + f, g, stride=2 * plan.tiles), :] = total

    for at in range(parts + 2):
        if at < parts:
            shift_and_start(at)
        if 0 <= at - 1 < parts:
            first(at - 1)
        if 0 <= at - 2 < parts:
            sweep_up(at - 2)
    swept[0] = jnp.zeros((m, LANES), jnp.float32)
    if owner:
        b_pad[plan.rows :, :] = jnp.zeros((plan.pad, LANES), jnp.float32)
    for at in range(parts + 2):
        if at < parts:
            sweep_down(parts - 1 - at)
        if 0 <= at - 1 < parts:
            last(parts - at)
        if 0 <= at - 2 < parts:
            end(parts + 1 - at)

    if owner:
        back = (LANES - roll) & (LANES - 1)
        from_here = tall(lane < LANES - roll)
        here = moved(b_pad, down, back)
        for t in range(plan.tiles):
            after = moved(b_pad, t + 1 + down, back)
            j, k = j_and_k(t)
            valid = tall((j < g - oy) & (k < g - oz))
            term = jnp.where(valid, jnp.where(from_here, here, after), 0.0)
            here = after
            if role == "visiting":
                out_ref[t] = term
                continue
            other, other_at = other_ref[t], other_e_ref[0, 0, 0, 1]
            for f in range(2):
                out_ref[f, t] = jnp.where(other_at == f, other, 0.0) + jnp.where(v_at == f, term, 0.0)
    if role == "last":
        out_ref[...] = both[...].astype(jnp.bfloat16)


def smem():
    return pl.BlockSpec(memory_space=pltpu.SMEM)


def vmem():
    return pl.BlockSpec(memory_space=pltpu.VMEM)


def params():
    return pltpu.CompilerParams(vmem_limit_bytes=VMEM_BYTES)


def cost(flops, size):
    return pl.CostEstimate(flops=flops, bytes_accessed=size, transcendentals=0)


def pick(step, e, w):
    return pl.pallas_call(
        functools.partial(pick_kernel, step),
        out_shape=jax.ShapeDtypeStruct(w.shape[1:], w.dtype),
        in_specs=[smem(), vmem()],
        out_specs=vmem(),
        compiler_params=params(),
        cost_estimate=cost(10**6, 10**6),
        name="pick",
    )(e, w)


def prepare(plan, e, raw):
    shape = jax.ShapeDtypeStruct((plan.rows, LANES), raw.dtype)
    hbm = pl.BlockSpec(memory_space=pltpu.HBM)
    return pl.pallas_call(
        functools.partial(prepare_kernel, plan, PREP_CHUNKS),
        out_shape=[jax.ShapeDtypeStruct((2, plan.rows, LANES), raw.dtype), shape, shape],
        in_specs=[hbm] * 2,
        out_specs=[vmem()] * 3,
        scratch_shapes=[
            pltpu.SMEM(e.shape, e.dtype),
            pltpu.VMEM(raw.shape, raw.dtype),
            pltpu.VMEM(raw.shape, jnp.float32),
            pltpu.SemaphoreType.DMA((PREP_CHUNKS + 1,)),
        ],
        compiler_params=pltpu.CompilerParams(vmem_limit_bytes=PREP_BYTES),
        cost_estimate=cost(10**6, 10**6),
        name="prepare",
    )(e, raw)


def make_tables(plan):
    g, m = plan.g, plan.modes
    shapes = (
        ((LANES, 2 * LANES), jnp.bfloat16),
        ((m, 3 * g), jnp.bfloat16),
        ((2 * g, 2 * m), jnp.bfloat16),
        ((2 * g, 2 * LANES), jnp.bfloat16),
        ((g, m, LANES), jnp.float32),
    )
    return pl.pallas_call(
        functools.partial(tables_kernel, plan),
        out_shape=[jax.ShapeDtypeStruct(*shape) for shape in shapes],
        out_specs=[vmem()] * len(shapes),
        compiler_params=params(),
        cost_estimate=cost(10**7, 10**6),
        name="tables",
    )()


def solve(plan, role, step, e, w, x, tables, extra=()):
    g, m = plan.g, plan.modes
    term = jax.ShapeDtypeStruct((plan.tiles, g, LANES), jnp.float32)
    out = {
        "visiting": term,
        "visiting_sum": jax.ShapeDtypeStruct((2,) + term.shape, term.dtype),
        "resident": term,
        "last": jax.ShapeDtypeStruct((2 * plan.rows, LANES), w.dtype),
    }[role]
    more = {"visiting_sum": [smem(), vmem()], "last": [vmem()] * 2}.get(role, [])
    return pl.pallas_call(
        functools.partial(solve_kernel, plan, role, step),
        out_shape=out,
        in_specs=[smem()] + [vmem()] * 7 + more,
        out_specs=vmem(),
        scratch_shapes=[
            pltpu.VMEM((plan.rows, LANES), jnp.float32),
            pltpu.VMEM((plan.rows + plan.pad, LANES), jnp.float32),
            pltpu.VMEM((plan.tiles, g, LANES), jnp.float32),
            pltpu.VMEM((g * g, LANES), jnp.bfloat16),
            pltpu.VMEM((g * g, LANES), jnp.bfloat16),
            pltpu.VMEM((g * g, LANES), jnp.bfloat16),
            pltpu.VMEM((g, m, LANES), jnp.float32),
            pltpu.VMEM((g * m, LANES), jnp.bfloat16),
            pltpu.VMEM((g * m, LANES), jnp.bfloat16),
            pltpu.VMEM((g * g, 2 * LANES), jnp.bfloat16),
        ]
        + ([pltpu.VMEM((2 * plan.rows, LANES), jnp.float32)] if role == "last" else []),
        compiler_params=params(),
        cost_estimate=cost(2 * 10**8, 4 * 10**6),
    )(e, w, x, *tables, *extra)


def per_device(wannier, pairs):
    plan = Plan(wannier.shape[1])
    count = lax.axis_size("blk")

    def shifted(array, by):
        return lax.ppermute(array, "blk", [(i, (i + by) % count) for i in range(count)])

    raw = wannier.reshape(2, plan.rows, LANES).transpose(1, 0, 2).reshape(2 * plan.rows, LANES)
    w, a1, a2 = prepare(plan, pairs, raw)
    e1 = shifted(pairs, -1)
    e2 = shifted(pairs, -2)
    a1 = shifted(a1, -1)
    a2 = shifted(a2, -2)
    b1 = pick(0, e1, w)
    b2 = pick(1, e2, w)
    b1 = shifted(b1, 1)
    b2 = shifted(b2, 2)
    tables = make_tables(plan)
    t1 = solve(plan, "visiting", 0, e1, w, a1, tables)
    partial = solve(plan, "visiting_sum", 1, e2, w, a2, tables, (e1, t1))
    r1 = solve(plan, "resident", 0, pairs, w, b1, tables)
    out = solve(plan, "last", 1, pairs, w, b2, tables, (partial, r1))
    out = out.reshape(plan.rows, 2, LANES).transpose(1, 0, 2)
    return out.reshape(wannier.shape)


def solution(mesh):
    return jax.shard_map(
        per_device,
        mesh=mesh,
        in_specs=(P("blk", None), P("blk", None, None, None)),
        out_specs=P("blk", None),
        check_vma=False,
    )
```

```python
import functools

import jax
import jax.numpy as jnp
import numpy as np
from jax import lax
from jax.experimental import pallas as pl
from jax.experimental.pallas import tpu as pltpu
from jax.sharding import PartitionSpec as P


LANES = 128
VMEM_BYTES = 20 * 1024 * 1024
PREP_BYTES = 20963328
PREP_CHUNKS = 4


class Plan:
    def __init__(self, points):
        self.g = g = round(points ** (1.0 / 3.0))
        assert g**3 == points and (g * g) % (2 * LANES) == 0 and g % 16 == 0
        self.modes = 2 * g
        assert self.modes <= LANES
        self.tiles = g * g // LANES
        self.rows = points // LANES
        half = g // 2
        self.pad = -(-(half * (g * g + g + 1) // LANES + 1) // 8) * 8


def split(x):
    hi = x.astype(jnp.bfloat16)
    lo = (x - hi.astype(jnp.float32)).astype(jnp.bfloat16)
    return hi, lo


def dot(a, b):
    return jnp.dot(a, b, preferred_element_type=jnp.float32)


def sine_table(shape, modes, row_end, lane_end):
    row = lax.broadcasted_iota(jnp.int32, shape, 0)
    lane = lax.broadcasted_iota(jnp.int32, shape, 1)
    period = 2 * (modes + 1)
    product = ((row + 1) * (lane + 1)).astype(jnp.float32)
    turns = jnp.floor((product + 0.5) * (1.0 / period))
    angle = (product - turns * period) * (np.pi / (modes + 1))
    sine = jnp.sin(angle) * np.sqrt(2.0 / (modes + 1.0))
    return jnp.where((row < row_end) & (lane < lane_end), sine, 0.0)


def tables_kernel(plan, start_ref, first_ref, last_ref, end_ref, ratio_ref):
    g, m = plan.g, plan.modes
    half = LANES // 2
    shape = (m, LANES)
    step = np.pi / (m + 1)
    row = lax.broadcasted_iota(jnp.int32, shape, 0).astype(jnp.float32)
    lane = lax.broadcasted_iota(jnp.int32, shape, 1).astype(jnp.float32)
    mu = 4.0 * (jnp.sin((row + 1.0) * (0.5 * step)) ** 2 + jnp.sin((lane + 1.0) * (0.5 * step)) ** 2)
    small = jnp.ones_like(mu)
    for j in range(g):
        before = small
        total = mu + small
        ratio = 1.0 / (1.0 + total)
        small = total * ratio
        if j == g - 1:
            ratio = 1.0 / (mu + before + small)
        ratio_ref[j] = ratio
    hi, lo = split(sine_table((m, LANES), m, m, g)[:, :g])
    first_ref[...] = jnp.concatenate([hi, hi, lo], axis=1)
    hi, lo = split(sine_table((g, LANES), m, g, m))
    gap = jnp.zeros((half - g, 2 * LANES), jnp.bfloat16)
    wide = jnp.concatenate([hi, lo], axis=1)
    start_ref[...] = jnp.concatenate([wide, gap, wide, gap], axis=0)
    end_ref[...] = jnp.concatenate(
        [jnp.concatenate([hi, hi], axis=1), jnp.concatenate([lo, lo], axis=1)], axis=0
    )
    hi, lo = hi[:, :m], lo[:, :m]
    last_ref[...] = jnp.concatenate(
        [jnp.concatenate([hi, hi], axis=1), jnp.concatenate([lo, lo], axis=1)], axis=0
    )


def prepare_kernel(plan, chunks, e_hbm, raw_hbm, w_ref, o1_ref, o2_ref, e_ref, raw_ref, both, sems):
    rows = plan.rows // chunks
    copies = [
        pltpu.make_async_copy(
            raw_hbm.at[pl.ds(2 * rows * at, 2 * rows)], raw_ref.at[pl.ds(2 * rows * at, 2 * rows)], sems.at[at]
        )
        for at in range(chunks)
    ]
    copies.append(pltpu.make_async_copy(e_hbm, e_ref, sems.at[chunks]))
    for copy in copies[-1:] + copies[:-1]:
        copy.start()
    copies[-1].wait()
    entries = e_ref[0, 0], e_ref[0, 1]
    first, second = [entry[0, 0] == 0 for entry in entries]
    for at in range(chunks):
        copies[at].wait()
        here = pl.ds(rows * at, rows)
        both[pl.ds(2 * rows * at, 2 * rows), :] = raw_ref[pl.ds(2 * rows * at, 2 * rows), :].astype(jnp.float32)
        f0, f1 = [both[pl.ds(2 * rows * at + f, rows, stride=2), :] for f in range(2)]
        w_ref[0, here, :] = f0.astype(jnp.bfloat16)
        w_ref[1, here, :] = f1.astype(jnp.bfloat16)
        o1_ref[here, :] = jnp.where(first, f0, f1).astype(jnp.bfloat16)
        o2_ref[here, :] = jnp.where(second, f0, f1).astype(jnp.bfloat16)


def pick_kernel(step, e_ref, w_ref, out_ref):
    entry = e_ref[0, step]
    out_ref[...] = w_ref[entry[0, 1]]


def solve_kernel(plan, role, step, *refs):
    owner = role.startswith("visiting")
    (e_ref, w_ref, x_ref, start_ref, first_ref, last_ref, end_ref, ratio_ref) = refs[:8]
    refs = refs[8:]
    if role == "visiting_sum":
        (other_e_ref, other_ref), refs = refs[:2], refs[2:]
        other_entry = other_e_ref[0, 0]
    if role == "last":
        (partial_ref, other_ref), refs = refs[:2], refs[2:]
        other_entry = e_ref[0, 0]
    out_ref, a_pad, b_pad, b_sh, rho_t, x_hi, x_lo, z, y_hi, y_lo, v = refs[:11]
    both = refs[11] if role == "last" else None
    g, m = plan.g, plan.modes
    entry = e_ref[0, step]
    r_at, v_at, ox, oy, oz, live = [entry[0, at] for at in range(6)]
    live = live.astype(jnp.float32)
    shift = ox * (g * g) + oy * g + oz
    down = lax.shift_right_logical(shift, 7)
    roll = shift & (LANES - 1)

    if owner:
        a_pad[: plan.rows, :] = x_ref[...].astype(jnp.float32)
        b_pad[plan.pad :, :] = w_ref[v_at].astype(jnp.float32)
    else:
        a_pad[: plan.rows, :] = w_ref[r_at].astype(jnp.float32)
        b_pad[plan.pad :, :] = x_ref[...].astype(jnp.float32)
    b_pad[: plan.pad, :] = jnp.zeros((plan.pad, LANES), jnp.float32)

    lane = lax.broadcasted_iota(jnp.int32, (8, LANES), 1)

    def j_and_k(t):
        flat = (lane + t * LANES).astype(jnp.float32)
        j = jnp.floor((flat + 0.5) * (1.0 / g))
        return j.astype(jnp.int32), (flat - j * g).astype(jnp.int32)

    def tall(x):
        return jnp.concatenate([x] * (g // 8), axis=0)

    def moved(ref, start, amount):
        return pltpu.roll(ref[pl.ds(start, g, stride=plan.tiles), :], amount, 1)

    from_before = tall(lane < roll)
    parts = 3
    js = g // parts
    tiles = plan.tiles // parts
    assert g % parts == 0 and js % 2 == 0 and plan.tiles % parts == 0 and tiles % 2 == 0
    last_rolled = [moved(b_pad, plan.pad - 1 - down, roll)]
    gap = jnp.zeros((LANES // 2 - g, LANES), jnp.bfloat16)

    def shift_and_start(part):
        for t in range(part * tiles, (part + 1) * tiles):
            before = last_rolled[0]
            here = moved(b_pad, plan.pad + t - down, roll)
            j, k = j_and_k(t)
            valid = tall((j >= oy) & (k >= oz))
            b = jnp.where(valid, jnp.where(from_before, before, here), 0.0)
            last_rolled[0] = here
            if not owner:
                b_sh[t] = b
            hi, lo = split(a_pad[pl.ds(t, g, stride=plan.tiles), :] * b)
            rho_t[pl.ds(t * LANES, LANES), :] = jnp.concatenate([hi, gap, lo, gap], axis=0).T
            if t % 2:
                rows = pl.ds((t - 1) * LANES, 2 * LANES)
                x = dot(rho_t[rows, :], start_ref[...])
                x_hi[rows, :], x_lo[rows, :] = split(x[:, :LANES] + x[:, LANES:])

    def beside(ref, j, rows):
        return jnp.concatenate([ref[pl.ds(j * rows, rows), :], ref[pl.ds((j + 1) * rows, rows), :]], axis=1)

    def first(part):
        for j in range(part * js, (part + 1) * js, 2):
            hi, lo = beside(x_hi, j, g), beside(x_lo, j, g)
            x = dot(first_ref[...], jnp.concatenate([hi, lo, hi], axis=0))
            z[j], z[j + 1] = x[:, :LANES], x[:, LANES:]

    swept = [None]

    def sweep_up(part):
        w = swept[0]
        for j in range(part * js, (part + 1) * js):
            w = z[j] if j == 0 else z[j] + ratio_ref[j - 1] * w
            z[j] = w
        swept[0] = w

    def sweep_down(part):
        y = swept[0]
        for j in reversed(range(part * js, (part + 1) * js)):
            y = ratio_ref[j] * (z[j] + y)
            y_hi[pl.ds(j * m, m), :], y_lo[pl.ds(j * m, m), :] = split(y)
        swept[0] = y

    def last(part):
        for j in reversed(range(part * js, (part + 1) * js, 2)):
            x = dot(last_ref[...], jnp.concatenate([beside(y_hi, j, m), beside(y_lo, j, m)], axis=0))
            hi, lo = split(x[:g] + x[g:])
            for side in range(2):
                rows = pl.ds((j + side) * g, g)
                lanes = slice(side * LANES, (side + 1) * LANES)
                v[rows, pl.ds(0, LANES)] = hi[:, lanes]
                v[rows, pl.ds(LANES, LANES)] = lo[:, lanes]

    def end(part):
        for pair in range(part * tiles // 2, (part + 1) * tiles // 2):
            pieces = lax.dot_general(
                end_ref[...],
                v[pl.ds(pair * 2 * LANES, 2 * LANES), :],
                (((1,), (1,)), ((), ())),
                preferred_element_type=jnp.float32,
            )
            phi2 = (pieces[:g] + pieces[g:]) * live
            for side in range(2):
                t = 2 * pair + side
                phi = phi2[:, side * LANES : (side + 1) * LANES]
                if owner:
                    b_pad[pl.ds(t, g, stride=plan.tiles), :] = phi * a_pad[pl.ds(t, g, stride=plan.tiles), :]
                elif role == "resident":
                    out_ref[t] = phi * b_sh[t]
                else:
                    own, other = phi * b_sh[t], other_ref[t]
                    other_at = other_entry[0, 0]
                    for f in range(2):
                        total = partial_ref[f, t]
                        total = total + jnp.where(other_at == f, other, 0.0) + jnp.where(r_at == f, own, 0.0)
                        both[pl.ds(2 * t + f, g, stride=2 * plan.tiles), :] = total

    for at in range(parts + 2):
        if at < parts:
            shift_and_start(at)
        if 0 <= at - 1 < parts:
            first(at - 1)
        if 0 <= at - 2 < parts:
            sweep_up(at - 2)
    swept[0] = jnp.zeros((m, LANES), jnp.float32)
    if owner:
        b_pad[plan.rows :, :] = jnp.zeros((plan.pad, LANES), jnp.float32)
    for at in range(parts + 2):
        if at < parts:
            sweep_down(parts - 1 - at)
        if 0 <= at - 1 < parts:
            last(parts - at)
        if 0 <= at - 2 < parts:
            end(parts + 1 - at)

    if owner:
        back = (LANES - roll) & (LANES - 1)
        from_here = tall(lane < LANES - roll)
        here = moved(b_pad, down, back)
        for t in range(plan.tiles):
            after = moved(b_pad, t + 1 + down, back)
            j, k = j_and_k(t)
            valid = tall((j < g - oy) & (k < g - oz))
            term = jnp.where(valid, jnp.where(from_here, here, after), 0.0)
            here = after
            if role == "visiting":
                out_ref[t] = term
                continue
            other, other_at = other_ref[t], other_entry[0, 1]
            for f in range(2):
                out_ref[f, t] = jnp.where(other_at == f, other, 0.0) + jnp.where(v_at == f, term, 0.0)
    if role == "last":
        out_ref[...] = both[...].astype(jnp.bfloat16)


def vmem():
    return pl.BlockSpec(memory_space=pltpu.VMEM)


def params():
    return pltpu.CompilerParams(vmem_limit_bytes=VMEM_BYTES)


def cost(flops, size):
    return pl.CostEstimate(flops=flops, bytes_accessed=size, transcendentals=0)


def pick(step, e, w):
    return pl.pallas_call(
        functools.partial(pick_kernel, step),
        out_shape=jax.ShapeDtypeStruct(w.shape[1:], w.dtype),
        in_specs=[vmem(), vmem()],
        out_specs=vmem(),
        compiler_params=params(),
        cost_estimate=cost(10**6, 10**6),
        name="pick",
    )(e, w)


def prepare(plan, e, raw):
    shape = jax.ShapeDtypeStruct((plan.rows, LANES), raw.dtype)
    hbm = pl.BlockSpec(memory_space=pltpu.HBM)
    return pl.pallas_call(
        functools.partial(prepare_kernel, plan, PREP_CHUNKS),
        out_shape=[
            jax.ShapeDtypeStruct((2, plan.rows, LANES), raw.dtype),
            shape,
            shape,
            jax.ShapeDtypeStruct(e.shape, e.dtype),
        ],
        in_specs=[hbm] * 2,
        out_specs=[vmem()] * 4,
        scratch_shapes=[
            pltpu.VMEM(raw.shape, raw.dtype),
            pltpu.VMEM(raw.shape, jnp.float32),
            pltpu.SemaphoreType.DMA((PREP_CHUNKS + 1,)),
        ],
        compiler_params=pltpu.CompilerParams(vmem_limit_bytes=PREP_BYTES),
        cost_estimate=cost(10**6, 10**6),
        name="prepare",
    )(e, raw)


def make_tables(plan):
    g, m = plan.g, plan.modes
    shapes = (
        ((LANES, 2 * LANES), jnp.bfloat16),
        ((m, 3 * g), jnp.bfloat16),
        ((2 * g, 2 * m), jnp.bfloat16),
        ((2 * g, 2 * LANES), jnp.bfloat16),
        ((g, m, LANES), jnp.float32),
    )
    return pl.pallas_call(
        functools.partial(tables_kernel, plan),
        out_shape=[jax.ShapeDtypeStruct(*shape) for shape in shapes],
        out_specs=[vmem()] * len(shapes),
        compiler_params=params(),
        cost_estimate=cost(10**7, 10**6),
        name="tables",
    )()


def solve(plan, role, step, e, w, x, tables, extra=()):
    g, m = plan.g, plan.modes
    term = jax.ShapeDtypeStruct((plan.tiles, g, LANES), jnp.float32)
    out = {
        "visiting": term,
        "visiting_sum": jax.ShapeDtypeStruct((2,) + term.shape, term.dtype),
        "resident": term,
        "last": jax.ShapeDtypeStruct((2 * plan.rows, LANES), w.dtype),
    }[role]
    more = {"visiting_sum": [vmem()] * 2, "last": [vmem()] * 2}.get(role, [])
    return pl.pallas_call(
        functools.partial(solve_kernel, plan, role, step),
        out_shape=out,
        in_specs=[vmem()] * 8 + more,
        out_specs=vmem(),
        scratch_shapes=[
            pltpu.VMEM((plan.rows, LANES), jnp.float32),
            pltpu.VMEM((plan.rows + plan.pad, LANES), jnp.float32),
            pltpu.VMEM((plan.tiles, g, LANES), jnp.float32),
            pltpu.VMEM((g * g, LANES), jnp.bfloat16),
            pltpu.VMEM((g * g, LANES), jnp.bfloat16),
            pltpu.VMEM((g * g, LANES), jnp.bfloat16),
            pltpu.VMEM((g, m, LANES), jnp.float32),
            pltpu.VMEM((g * m, LANES), jnp.bfloat16),
            pltpu.VMEM((g * m, LANES), jnp.bfloat16),
            pltpu.VMEM((g * g, 2 * LANES), jnp.bfloat16),
        ]
        + ([pltpu.VMEM((2 * plan.rows, LANES), jnp.float32)] if role == "last" else []),
        compiler_params=params(),
        cost_estimate=cost(2 * 10**8, 4 * 10**6),
    )(e, w, x, *tables, *extra)


def per_device(wannier, pairs):
    plan = Plan(wannier.shape[1])
    count = lax.axis_size("blk")

    def shifted(array, by):
        return lax.ppermute(array, "blk", [(i, (i + by) % count) for i in range(count)])

    raw = wannier.reshape(2, plan.rows, LANES).transpose(1, 0, 2).reshape(2 * plan.rows, LANES)
    w, a1, a2, own = prepare(plan, pairs, raw)
    e1 = shifted(pairs, -1)
    e2 = shifted(pairs, -2)
    a1 = shifted(a1, -1)
    a2 = shifted(a2, -2)
    b1 = pick(0, e1, w)
    b2 = pick(1, e2, w)
    b1 = shifted(b1, 1)
    b2 = shifted(b2, 2)
    tables = make_tables(plan)
    t1 = solve(plan, "visiting", 0, e1, w, a1, tables)
    partial = solve(plan, "visiting_sum", 1, e2, w, a2, tables, (e1, t1))
    r1 = solve(plan, "resident", 0, own, w, b1, tables)
    out = solve(plan, "last", 1, own, w, b2, tables, (partial, r1))
    out = out.reshape(plan.rows, 2, LANES).transpose(1, 0, 2)
    return out.reshape(wannier.shape)


def solution(mesh):
    return jax.shard_map(
        per_device,
        mesh=mesh,
        in_specs=(P("blk", None), P("blk", None, None, None)),
        out_specs=P("blk", None),
        check_vma=False,
    )
```

```python
import functools

import jax
import jax.numpy as jnp
import numpy as np
from jax import lax
from jax.experimental import pallas as pl
from jax.experimental.pallas import tpu as pltpu
from jax.sharding import PartitionSpec as P


LANES = 128
VMEM_BYTES = 20 * 1024 * 1024
PREP_BYTES = 20963328
PREP_CHUNKS = 4
LAST_BYTES = 32 * 1024 * 1024
LEAD = 3


class Plan:
    def __init__(self, points):
        self.g = g = round(points ** (1.0 / 3.0))
        assert g**3 == points and (g * g) % (2 * LANES) == 0 and g % 16 == 0
        self.modes = 2 * g
        assert self.modes <= LANES
        self.tiles = g * g // LANES
        self.rows = points // LANES
        half = g // 2
        self.pad = -(-(half * (g * g + g + 1) // LANES + 1) // 8) * 8


def split(x):
    hi = x.astype(jnp.bfloat16)
    lo = (x - hi.astype(jnp.float32)).astype(jnp.bfloat16)
    return hi, lo


def dot(a, b):
    return jnp.dot(a, b, preferred_element_type=jnp.float32)


def sine_table(shape, modes, row_end, lane_end):
    row = lax.broadcasted_iota(jnp.int32, shape, 0)
    lane = lax.broadcasted_iota(jnp.int32, shape, 1)
    period = 2 * (modes + 1)
    product = ((row + 1) * (lane + 1)).astype(jnp.float32)
    turns = jnp.floor((product + 0.5) * (1.0 / period))
    angle = (product - turns * period) * (np.pi / (modes + 1))
    sine = jnp.sin(angle) * np.sqrt(2.0 / (modes + 1.0))
    return jnp.where((row < row_end) & (lane < lane_end), sine, 0.0)


def tables_kernel(plan, start_ref, first_ref, last_ref, end_ref, ratio_ref):
    g, m = plan.g, plan.modes
    half = LANES // 2
    shape = (m, LANES)
    step = np.pi / (m + 1)
    row = lax.broadcasted_iota(jnp.int32, shape, 0).astype(jnp.float32)
    lane = lax.broadcasted_iota(jnp.int32, shape, 1).astype(jnp.float32)
    mu = 4.0 * (jnp.sin((row + 1.0) * (0.5 * step)) ** 2 + jnp.sin((lane + 1.0) * (0.5 * step)) ** 2)
    small = jnp.ones_like(mu)
    for j in range(g):
        before = small
        total = mu + small
        ratio = 1.0 / (1.0 + total)
        small = total * ratio
        if j == g - 1:
            ratio = 1.0 / (mu + before + small)
        ratio_ref[j] = ratio
    hi, lo = split(sine_table((m, LANES), m, m, g)[:, :g])
    first_ref[...] = jnp.concatenate([hi, hi, lo], axis=1)
    hi, lo = split(sine_table((g, LANES), m, g, m))
    gap = jnp.zeros((half - g, 2 * LANES), jnp.bfloat16)
    wide = jnp.concatenate([hi, lo], axis=1)
    start_ref[...] = jnp.concatenate([wide, gap, wide, gap], axis=0)
    end_ref[...] = jnp.concatenate(
        [jnp.concatenate([hi, hi], axis=1), jnp.concatenate([lo, lo], axis=1)], axis=0
    )
    hi, lo = hi[:, :m], lo[:, :m]
    last_ref[...] = jnp.concatenate(
        [jnp.concatenate([hi, hi], axis=1), jnp.concatenate([lo, lo], axis=1)], axis=0
    )


def prepare_kernel(plan, chunks, e_hbm, raw_hbm, w_ref, o1_ref, o2_ref, e_ref, raw_ref, both, sems):
    rows = plan.rows // chunks
    copies = [
        pltpu.make_async_copy(
            raw_hbm.at[pl.ds(2 * rows * at, 2 * rows)], raw_ref.at[pl.ds(2 * rows * at, 2 * rows)], sems.at[at]
        )
        for at in range(chunks)
    ]
    copies.append(pltpu.make_async_copy(e_hbm, e_ref, sems.at[chunks]))
    for copy in copies[-1:] + copies[:-1]:
        copy.start()
    copies[-1].wait()
    entries = e_ref[0, 0], e_ref[0, 1]
    first, second = [entry[0, 0] == 0 for entry in entries]
    for at in range(chunks):
        copies[at].wait()
        here = pl.ds(rows * at, rows)
        both[pl.ds(2 * rows * at, 2 * rows), :] = raw_ref[pl.ds(2 * rows * at, 2 * rows), :].astype(jnp.float32)
        f0, f1 = [both[pl.ds(2 * rows * at + f, rows, stride=2), :] for f in range(2)]
        w_ref[0, here, :] = f0.astype(jnp.bfloat16)
        w_ref[1, here, :] = f1.astype(jnp.bfloat16)
        o1_ref[here, :] = jnp.where(first, f0, f1).astype(jnp.bfloat16)
        o2_ref[here, :] = jnp.where(second, f0, f1).astype(jnp.bfloat16)


def pick_kernel(step, e_ref, w_ref, out_ref):
    entry = e_ref[0, step]
    out_ref[...] = w_ref[entry[0, 1]]


def solve_steps(plan, role, step, *refs):
    owner = role.startswith("visiting")
    (e_ref, w_ref, x_ref, start_ref, first_ref, last_ref, end_ref, ratio_ref) = refs[:8]
    refs = refs[8:]
    if role == "visiting_sum":
        (other_e_ref, other_ref), refs = refs[:2], refs[2:]
        other_entry = other_e_ref[0, 0]
    if role == "last":
        (partial_ref, other_ref), refs = refs[:2], refs[2:]
        other_entry = e_ref[0, 0]
    out_ref, a_pad, b_pad, b_sh, rho_t, x_hi, x_lo, z, y_hi, y_lo, v = refs[:11]
    both = refs[11] if role == "last" else None
    g, m = plan.g, plan.modes
    entry = e_ref[0, step]
    r_at, v_at, ox, oy, oz, live = [entry[0, at] for at in range(6)]
    live = live.astype(jnp.float32)
    shift = ox * (g * g) + oy * g + oz
    down = lax.shift_right_logical(shift, 7)
    roll = shift & (LANES - 1)

    if owner:
        a_pad[: plan.rows, :] = x_ref[...].astype(jnp.float32)
        b_pad[plan.pad :, :] = w_ref[v_at].astype(jnp.float32)
    else:
        a_pad[: plan.rows, :] = w_ref[r_at].astype(jnp.float32)
        b_pad[plan.pad :, :] = x_ref[...].astype(jnp.float32)
    b_pad[: plan.pad, :] = jnp.zeros((plan.pad, LANES), jnp.float32)

    lane = lax.broadcasted_iota(jnp.int32, (8, LANES), 1)

    def j_and_k(t):
        flat = (lane + t * LANES).astype(jnp.float32)
        j = jnp.floor((flat + 0.5) * (1.0 / g))
        return j.astype(jnp.int32), (flat - j * g).astype(jnp.int32)

    def tall(x):
        return jnp.concatenate([x] * (g // 8), axis=0)

    def moved(ref, start, amount):
        return pltpu.roll(ref[pl.ds(start, g, stride=plan.tiles), :], amount, 1)

    from_before = tall(lane < roll)
    parts = 3
    js = g // parts
    tiles = plan.tiles // parts
    assert g % parts == 0 and js % 2 == 0 and plan.tiles % parts == 0 and tiles % 2 == 0
    last_rolled = [moved(b_pad, plan.pad - 1 - down, roll)]
    gap = jnp.zeros((LANES // 2 - g, LANES), jnp.bfloat16)

    def shift_and_start(part):
        for t in range(part * tiles, (part + 1) * tiles):
            before = last_rolled[0]
            here = moved(b_pad, plan.pad + t - down, roll)
            j, k = j_and_k(t)
            valid = tall((j >= oy) & (k >= oz))
            b = jnp.where(valid, jnp.where(from_before, before, here), 0.0)
            last_rolled[0] = here
            if not owner:
                b_sh[t] = b
            hi, lo = split(a_pad[pl.ds(t, g, stride=plan.tiles), :] * b)
            rho_t[pl.ds(t * LANES, LANES), :] = jnp.concatenate([hi, gap, lo, gap], axis=0).T
            if t % 2:
                rows = pl.ds((t - 1) * LANES, 2 * LANES)
                x = dot(rho_t[rows, :], start_ref[...])
                x_hi[rows, :], x_lo[rows, :] = split(x[:, :LANES] + x[:, LANES:])

    def beside(ref, j, rows):
        return jnp.concatenate([ref[pl.ds(j * rows, rows), :], ref[pl.ds((j + 1) * rows, rows), :]], axis=1)

    def first(part):
        for j in range(part * js, (part + 1) * js, 2):
            hi, lo = beside(x_hi, j, g), beside(x_lo, j, g)
            x = dot(first_ref[...], jnp.concatenate([hi, lo, hi], axis=0))
            z[j], z[j + 1] = x[:, :LANES], x[:, LANES:]

    swept = [None]

    def sweep_up(part):
        w = swept[0]
        for j in range(part * js, (part + 1) * js):
            w = z[j] if j == 0 else z[j] + ratio_ref[j - 1] * w
            z[j] = w
        swept[0] = w

    def sweep_down(part):
        y = swept[0]
        for j in reversed(range(part * js, (part + 1) * js)):
            y = ratio_ref[j] * (z[j] + y)
            y_hi[pl.ds(j * m, m), :], y_lo[pl.ds(j * m, m), :] = split(y)
        swept[0] = y

    def last(part):
        for j in reversed(range(part * js, (part + 1) * js, 2)):
            x = dot(last_ref[...], jnp.concatenate([beside(y_hi, j, m), beside(y_lo, j, m)], axis=0))
            hi, lo = split(x[:g] + x[g:])
            for side in range(2):
                rows = pl.ds((j + side) * g, g)
                lanes = slice(side * LANES, (side + 1) * LANES)
                v[rows, pl.ds(0, LANES)] = hi[:, lanes]
                v[rows, pl.ds(LANES, LANES)] = lo[:, lanes]

    def end(part):
        for pair in range(part * tiles // 2, (part + 1) * tiles // 2):
            pieces = lax.dot_general(
                end_ref[...],
                v[pl.ds(pair * 2 * LANES, 2 * LANES), :],
                (((1,), (1,)), ((), ())),
                preferred_element_type=jnp.float32,
            )
            phi2 = (pieces[:g] + pieces[g:]) * live
            for side in range(2):
                t = 2 * pair + side
                phi = phi2[:, side * LANES : (side + 1) * LANES]
                if owner:
                    b_pad[pl.ds(t, g, stride=plan.tiles), :] = phi * a_pad[pl.ds(t, g, stride=plan.tiles), :]
                elif role == "resident":
                    out_ref[t] = phi * b_sh[t]
                else:
                    own, other = phi * b_sh[t], other_ref[t]
                    other_at = other_entry[0, 0]
                    for f in range(2):
                        total = partial_ref[f, t]
                        total = total + jnp.where(other_at == f, other, 0.0) + jnp.where(r_at == f, own, 0.0)
                        both[pl.ds(2 * t + f, g, stride=2 * plan.tiles), :] = total

    for at in range(parts + 2):
        if at < parts:
            shift_and_start(at)
        if 0 <= at - 1 < parts:
            first(at - 1)
        if 0 <= at - 2 < parts:
            sweep_up(at - 2)
        yield
    swept[0] = jnp.zeros((m, LANES), jnp.float32)
    if owner:
        b_pad[plan.rows :, :] = jnp.zeros((plan.pad, LANES), jnp.float32)
    for at in range(parts + 2):
        if at < parts:
            sweep_down(parts - 1 - at)
        if 0 <= at - 1 < parts:
            last(parts - at)
        if 0 <= at - 2 < parts:
            end(parts + 1 - at)
        yield

    if owner:
        back = (LANES - roll) & (LANES - 1)
        from_here = tall(lane < LANES - roll)
        here = moved(b_pad, down, back)
        for t in range(plan.tiles):
            after = moved(b_pad, t + 1 + down, back)
            j, k = j_and_k(t)
            valid = tall((j < g - oy) & (k < g - oz))
            term = jnp.where(valid, jnp.where(from_here, here, after), 0.0)
            here = after
            if role == "visiting":
                out_ref[t] = term
                continue
            other, other_at = other_ref[t], other_entry[0, 1]
            for f in range(2):
                out_ref[f, t] = jnp.where(other_at == f, other, 0.0) + jnp.where(v_at == f, term, 0.0)
    if role == "last":
        out_ref[...] = both[...].astype(jnp.bfloat16)


def solve_kernel(plan, role, step, *refs):
    for _ in solve_steps(plan, role, step, *refs):
        pass


def middle_kernel(plan, e2_ref, e1_ref, own_ref, w_ref, x1_ref, x2_ref, *refs):
    tables, (t1_ref, partial_ref, term_ref), refs = refs[:5], refs[5:8], refs[8:]
    early = solve_steps(
        plan, "visiting_sum", 1, e2_ref, w_ref, x1_ref, *tables, e1_ref, t1_ref, partial_ref, *refs[:10]
    )
    late = solve_steps(plan, "resident", 0, own_ref, w_ref, x2_ref, *tables, term_ref, *refs[10:])
    for _ in range(LEAD):
        next(early)
    for _ in early:
        next(late)
    for _ in late:
        pass


def vmem():
    return pl.BlockSpec(memory_space=pltpu.VMEM)


def params():
    return pltpu.CompilerParams(vmem_limit_bytes=VMEM_BYTES)


def cost(flops, size):
    return pl.CostEstimate(flops=flops, bytes_accessed=size, transcendentals=0)


def pick(step, e, w):
    return pl.pallas_call(
        functools.partial(pick_kernel, step),
        out_shape=jax.ShapeDtypeStruct(w.shape[1:], w.dtype),
        in_specs=[vmem(), vmem()],
        out_specs=vmem(),
        compiler_params=params(),
        cost_estimate=cost(10**6, 10**6),
        name="pick",
    )(e, w)


def prepare(plan, e, raw):
    shape = jax.ShapeDtypeStruct((plan.rows, LANES), raw.dtype)
    hbm = pl.BlockSpec(memory_space=pltpu.HBM)
    return pl.pallas_call(
        functools.partial(prepare_kernel, plan, PREP_CHUNKS),
        out_shape=[
            jax.ShapeDtypeStruct((2, plan.rows, LANES), raw.dtype),
            shape,
            shape,
            jax.ShapeDtypeStruct(e.shape, e.dtype),
        ],
        in_specs=[hbm] * 2,
        out_specs=[vmem()] * 4,
        scratch_shapes=[
            pltpu.VMEM(raw.shape, raw.dtype),
            pltpu.VMEM(raw.shape, jnp.float32),
            pltpu.SemaphoreType.DMA((PREP_CHUNKS + 1,)),
        ],
        compiler_params=pltpu.CompilerParams(vmem_limit_bytes=PREP_BYTES),
        cost_estimate=cost(10**6, 10**6),
        name="prepare",
    )(e, raw)


def make_tables(plan):
    g, m = plan.g, plan.modes
    shapes = (
        ((LANES, 2 * LANES), jnp.bfloat16),
        ((m, 3 * g), jnp.bfloat16),
        ((2 * g, 2 * m), jnp.bfloat16),
        ((2 * g, 2 * LANES), jnp.bfloat16),
        ((g, m, LANES), jnp.float32),
    )
    return pl.pallas_call(
        functools.partial(tables_kernel, plan),
        out_shape=[jax.ShapeDtypeStruct(*shape) for shape in shapes],
        out_specs=[vmem()] * len(shapes),
        compiler_params=params(),
        cost_estimate=cost(10**7, 10**6),
        name="tables",
    )()


def solve_scratch(plan):
    g, m = plan.g, plan.modes
    return [
        pltpu.VMEM((plan.rows, LANES), jnp.float32),
        pltpu.VMEM((plan.rows + plan.pad, LANES), jnp.float32),
        pltpu.VMEM((plan.tiles, g, LANES), jnp.float32),
        pltpu.VMEM((g * g, LANES), jnp.bfloat16),
        pltpu.VMEM((g * g, LANES), jnp.bfloat16),
        pltpu.VMEM((g * g, LANES), jnp.bfloat16),
        pltpu.VMEM((g, m, LANES), jnp.float32),
        pltpu.VMEM((g * m, LANES), jnp.bfloat16),
        pltpu.VMEM((g * m, LANES), jnp.bfloat16),
        pltpu.VMEM((g * g, 2 * LANES), jnp.bfloat16),
    ]


def solve_middle(plan, e2, e1, own, w, x1, x2, tables, t1):
    term = jax.ShapeDtypeStruct((plan.tiles, plan.g, LANES), jnp.float32)
    return pl.pallas_call(
        functools.partial(middle_kernel, plan),
        out_shape=[jax.ShapeDtypeStruct((2,) + term.shape, term.dtype), term],
        in_specs=[vmem()] * 12,
        out_specs=[vmem()] * 2,
        scratch_shapes=solve_scratch(plan) * 2,
        compiler_params=pltpu.CompilerParams(vmem_limit_bytes=LAST_BYTES),
        cost_estimate=cost(4 * 10**8, 8 * 10**6),
        name="solve_middle",
    )(e2, e1, own, w, x1, x2, *tables, t1)


def solve(plan, role, step, e, w, x, tables, extra=()):
    g = plan.g
    term = jax.ShapeDtypeStruct((plan.tiles, g, LANES), jnp.float32)
    out = {
        "visiting": term,
        "visiting_sum": jax.ShapeDtypeStruct((2,) + term.shape, term.dtype),
        "resident": term,
        "last": jax.ShapeDtypeStruct((2 * plan.rows, LANES), w.dtype),
    }[role]
    more = {"visiting_sum": [vmem()] * 2, "last": [vmem()] * 2}.get(role, [])
    return pl.pallas_call(
        functools.partial(solve_kernel, plan, role, step),
        out_shape=out,
        in_specs=[vmem()] * 8 + more,
        out_specs=vmem(),
        scratch_shapes=solve_scratch(plan)
        + ([pltpu.VMEM((2 * plan.rows, LANES), jnp.float32)] if role == "last" else []),
        compiler_params=params(),
        cost_estimate=cost(2 * 10**8, 4 * 10**6),
    )(e, w, x, *tables, *extra)


def per_device(wannier, pairs):
    plan = Plan(wannier.shape[1])
    count = lax.axis_size("blk")

    def shifted(array, by):
        return lax.ppermute(array, "blk", [(i, (i + by) % count) for i in range(count)])

    raw = wannier.reshape(2, plan.rows, LANES).transpose(1, 0, 2).reshape(2 * plan.rows, LANES)
    w, a1, a2, own = prepare(plan, pairs, raw)
    e1 = shifted(pairs, -1)
    e2 = shifted(pairs, -2)
    a1 = shifted(a1, -1)
    a2 = shifted(a2, -2)
    b1 = pick(0, e1, w)
    b2 = pick(1, e2, w)
    b1 = shifted(b1, 1)
    b2 = shifted(b2, 2)
    tables = make_tables(plan)
    t1 = solve(plan, "visiting", 0, e1, w, a1, tables)
    partial, r1 = solve_middle(plan, e2, e1, own, w, a2, b1, tables, t1)
    out = solve(plan, "last", 1, own, w, b2, tables, (partial, r1))
    out = out.reshape(plan.rows, 2, LANES).transpose(1, 0, 2)
    return out.reshape(wannier.shape)


def solution(mesh):
    return jax.shard_map(
        per_device,
        mesh=mesh,
        in_specs=(P("blk", None), P("blk", None, None, None)),
        out_specs=P("blk", None),
        check_vma=False,
    )
```
